256 devices in a mesh: box: 16 (over z, core), angle: 16 (over x, y).
Axes of the slice: x: 4, y: 4, z: 8, core: 2. Of those that a mesh axis runs over, the one named last changes fastest.
Arguments:
- coefficients: bfloat16 [2, 625, 98304], P(None, None, ('box', 'angle')), may hold values from -6 to 6
- plane_map: bfloat16 [2, 625, 2048], P(None, None, 'angle'), may hold values from -0.15625 to 0.15625
- leaf_parent: int32 [98304], P('box'), may hold values from -1 to 768, as said below
- leaf_octant: int32 [98304], P('box'), may hold values from 0 to 7, as said below
- box_parent: int32 [12288], P('box'), may hold values from -1 to 96, as said below
- box_octant: int32 [12288], P('box'), may hold values from 0 to 7, as said below
- interp_one: float32 [4, 4096], P(None, 'angle'), may hold values from 0.05 to 0.6
- phase_one: float32 [8, 4096], P(None, 'angle'), may hold values from -3.140625 to 3.140625
- interp_two: float32 [4, 8192], P(None, 'angle'), may hold values from 0.05 to 0.6
- phase_two: float32 [8, 8192], P(None, 'angle'), may hold values from -3.140625 to 3.140625
Outputs:
- signature_one: float32 [12288, 2, 4096], P('box', None, 'angle')
- signature_two: float32 [1536, 2, 8192], P('box', None, 'angle')
The draws below stay inside these ranges and needn't reach their ends.
Inputs may be any that keep to these rules, and one draw needn't show every extreme that they name: `leaf_parent`: within each block of 6144 leaf slots: the slots with -1 come first, then live slots whose values never fall and name every slot from 0 to the block's live level-1 count minus 1, then slots with 768. Counting its children in both blocks, each level-1 box has 4 to 7 children. In every block but the last, the last live level-1 box has children in the next block, which hold that block's -1 slots; the first block has no -1 slot. A level-1 slot is named by some leaf exactly when its box_parent is not 96. `leaf_octant`: the children of one parent have distinct octants, rising along the slots; empty slots hold 0. `box_parent`: within each block of 768 level-1 slots: the slots with -1 come first, then live slots whose values never fall and name every slot from 0 to the block's level-2 count minus 1, then slots with 96. Counting its children in both blocks, each level-2 box has 4 to 7 children. In every block but the last, the last live level-2 box has children in the next block, which hold that block's -1 slots; the first block has no -1 slot. Some block uses all 96 level-2 slots. `box_octant`: the children of one parent have distinct octants, rising along the slots; empty slots hold 0.
All inputs are finite; a program needn't handle non-finite values.
Results may differ from the reference program's by a relative error of at most 0.0029.
Values may be sent and summed in bfloat16 or wider, within the bound.
No kernel may reach another device: no remote copies, remote signals or barrier semaphores. Data moves between devices by JAX's collectives and lax.ppermute only.
A program may use at most 128 MiB of HBM per device.

```python
from functools import partial
import jax
import jax.numpy as jnp
from jax import lax

NC = 625
S0 = 2048
S1 = 4096
S2 = 8192
LEAF_DEV = 6144
LEAVES = 98304


def subset_table(key, group_sizes):
    scores = jax.random.randint(key, group_sizes.shape + (8,), 0, 1 << 20) * 8 + jnp.arange(8, dtype=jnp.int32)
    order = jnp.argsort(scores, axis=-1).astype(jnp.int32)
    masked = jnp.where(jnp.arange(8, dtype=jnp.int32) < group_sizes[..., None], order, 8)
    return jnp.sort(masked, axis=-1)


def place_slots(group_sizes, lead, total, prev_start, table, prev_row, slots, empty):
    ends = jnp.cumsum(group_sizes)
    starts = ends - group_sizes
    index = jnp.arange(slots, dtype=jnp.int32)
    offset = index - lead
    group = jnp.searchsorted(ends, offset, side='right').astype(jnp.int32)
    group = jnp.clip(group, 0, group_sizes.shape[0] - 1)
    position = jnp.clip(offset - starts[group], 0, 7)
    own_octant = table[group, position]
    lead_octant = prev_row[jnp.clip(prev_start + index, 0, 7)]
    parent = jnp.where(index < lead, -1, jnp.where(index < total, group, empty))
    octant = jnp.where(index < lead, lead_octant, jnp.where(index < total, own_octant, 0))
    return (parent.astype(jnp.int32), octant.astype(jnp.int32))


def build_level(key, groups, width, slots, empty, n_dev):
    key_sizes, key_tail, key_table = jax.random.split(key, 3)
    group_sizes = jax.random.randint(key_sizes, (n_dev, width), 4, 8)
    group_sizes = jnp.where(jnp.arange(width, dtype=jnp.int32)[None, :] < groups[:, None], group_sizes, 0)
    devices = jnp.arange(n_dev, dtype=jnp.int32)
    last_size = group_sizes[devices, groups - 1]
    tail = jax.random.randint(key_tail, (n_dev,), 1, last_size)
    tail = jnp.where(devices == n_dev - 1, 0, tail)
    lead = jnp.concatenate([jnp.zeros((1,), jnp.int32), tail[:-1]])
    total = lead + jnp.sum(group_sizes, axis=1) - tail
    table = subset_table(key_table, group_sizes)
    prev_row = jnp.roll(table[devices, groups - 1], 1, axis=0)
    prev_start = jnp.roll(last_size - tail, 1)
    placer = partial(place_slots, slots=slots, empty=empty)
    parent, octant = jax.vmap(placer)(group_sizes, lead, total, prev_start, table, prev_row)
    return (parent.reshape(-1), octant.reshape(-1), total)


def build_tree(key):
    n_dev = LEAVES // LEAF_DEV
    slots_one = LEAF_DEV // 8
    slots_two = LEAF_DEV // 64
    key_count, key_busy, key_upper, key_lower = jax.random.split(jax.random.fold_in(key, 4242), 4)
    groups = jax.random.randint(key_count, (n_dev,), 3 * slots_two // 4, slots_two + 1)
    busiest = jax.random.randint(key_busy, (), 0, n_dev)
    groups = jnp.where(jnp.arange(n_dev, dtype=jnp.int32) == busiest, slots_two, groups)
    box_parent, box_octant, owned = build_level(key_upper, groups, slots_two, slots_one, slots_two, n_dev)
    leaf_parent, leaf_octant, unused_total = build_level(key_lower, owned, slots_one, LEAF_DEV, slots_one, n_dev)
    return (leaf_parent, leaf_octant, box_parent, box_octant)


def draw_leaf_parent(key, part):
    return build_tree(key)[0]


def draw_leaf_octant(key, part):
    return build_tree(key)[1]


def draw_box_parent(key, part):
    return build_tree(key)[2]


def draw_box_octant(key, part):
    return build_tree(key)[3]


def level_of(own_key, shape, cuts, smallest, high):
    def one(axis_at, parts):
        heights = jax.random.uniform(jax.random.fold_in(jax.random.fold_in(own_key, 6), axis_at), (parts,), jnp.float32, smallest / len(cuts), high / len(cuts))
        return jnp.repeat(jnp.exp(heights), shape[axis_at] // parts).reshape((-1,) + (1,) * (len(shape) - axis_at - 1))

    level = one(*cuts[0])
    for cut in cuts[1:]:
        level = level * one(*cut)
    return level


def centred(rng, extent, deviation, reach, pieces=(), kind=jnp.bfloat16):
    loudness = level_of(rng, extent, pieces, -0.22, 0.18) if pieces else 1.0
    drawn = jax.random.normal(rng, extent, jnp.float32) * deviation * loudness
    return jnp.minimum(jnp.maximum(drawn, -reach), reach).astype(kind)


def setup_inputs(seed: int = 0) -> dict:
    seeds = jax.random.split(jax.random.key(seed), 11)
    return {
        "coefficients": centred(seeds[0], (2, NC, LEAVES), 1.0, 6.0, ((2, 256),)),
        "plane_map": centred(seeds[1], (2, NC, S0), (2 * NC) ** -0.5, 0.15625, ((2, 16),)),
        "leaf_parent": draw_leaf_parent(jax.random.fold_in(seeds[10], 71), 0),
        "leaf_octant": draw_leaf_octant(jax.random.fold_in(seeds[10], 71), 0),
        "box_parent": draw_box_parent(jax.random.fold_in(seeds[10], 71), 0),
        "box_octant": draw_box_octant(jax.random.fold_in(seeds[10], 71), 0),
        "interp_one": jnp.clip(0.05 + 0.55 * jax.random.uniform(seeds[6], (4, S1), jnp.float32) ** level_of(seeds[6], (4, S1), ((1, 16),), -0.2, 0.2), 0.05, 0.6),
        "phase_one": jnp.clip(jax.random.uniform(seeds[7], (8, S1), jnp.float32, -3.140625, 3.140625), -3.140625, 3.140625),
        "interp_two": jnp.clip(0.05 + 0.55 * jax.random.uniform(seeds[8], (4, S2), jnp.float32) ** level_of(seeds[8], (4, S2), ((1, 16),), -0.2, 0.2), 0.05, 0.6),
        "phase_two": jnp.clip(jax.random.uniform(seeds[9], (8, S2), jnp.float32, -3.140625, 3.140625), -3.140625, 3.140625),
    }


def real_form(block):
    real_part = block[0]
    imag_part = block[1]
    upper = jnp.concatenate([real_part, imag_part], axis=1)
    lower = jnp.concatenate([-imag_part, real_part], axis=1)
    return jnp.concatenate([upper, lower], axis=0)


def leaf_product(coef_block, weights):
    count = coef_block.shape[2]
    width = weights.shape[1] // 2
    flat = coef_block.reshape(coef_block.shape[0] * coef_block.shape[1], count)
    product = lax.dot_general(flat, weights, (((0,), (0,)), ((), ())), preferred_element_type=jnp.float32)
    return product.reshape(count, 2, width).astype(jnp.bfloat16)


def octant_rows(octant, table):
    selector = (octant[:, None] == jnp.arange(8, dtype=jnp.int32)[None, :]).astype(jnp.float32)
    return jnp.dot(selector, table, precision=lax.Precision.HIGHEST)


def upsample_shift(padded, weights, octant, cosine, sine):
    width = padded.shape[-1] - 4
    total = jnp.zeros(padded.shape[:-1] + (2 * width,), jnp.float32)
    for tap_index in range(4):
        window = padded[..., 1 + tap_index:1 + tap_index + width].astype(jnp.float32)
        total = total + weights[tap_index] * jnp.repeat(window, 2, axis=-1)
    cos_rows = octant_rows(octant, cosine)
    sin_rows = octant_rows(octant, sine)
    real_part = total[:, 0]
    imag_part = total[:, 1]
    return jnp.stack([real_part * cos_rows - imag_part * sin_rows,
                      real_part * sin_rows + imag_part * cos_rows], axis=1)


def wrap_pad(field):
    return jnp.concatenate([field[..., -2:], field, field[..., :2]], axis=-1)


def attach(owned, carried, last_slot):
    incoming = jnp.concatenate([carried[1:], jnp.zeros_like(carried[:1])], axis=0)
    slot_ids = jnp.arange(owned.shape[1], dtype=jnp.int32)
    selector = (slot_ids[None, :] == last_slot[:, None]).astype(jnp.float32)
    return owned + selector[:, :, None, None] * incoming[:, None]


def reference(coefficients, plane_map, leaf_parent, leaf_octant, box_parent, box_octant, interp_one, phase_one, interp_two, phase_two):
    n_dev = leaf_parent.shape[0] // LEAF_DEV
    slots_one = LEAF_DEV // 8
    slots_two = LEAF_DEV // 64
    weights = real_form(plane_map)
    cos_one = jnp.cos(phase_one)
    sin_one = jnp.sin(phase_one)
    cos_two = jnp.cos(phase_two)
    sin_two = jnp.sin(phase_two)
    parents_one = box_parent.reshape(n_dev, slots_one)
    octants_one = box_octant.reshape(n_dev, slots_one)

    def level_leaves(device):
        first = (device * LEAF_DEV).astype(jnp.int32)
        coef_block = lax.dynamic_slice_in_dim(coefficients, first, LEAF_DEV, 2)
        signature = leaf_product(coef_block, weights)
        parent = lax.dynamic_slice_in_dim(leaf_parent, first, LEAF_DEV, 0)
        octant = lax.dynamic_slice_in_dim(leaf_octant, first, LEAF_DEV, 0)
        contrib = upsample_shift(wrap_pad(signature), interp_one, octant, cos_one, sin_one)
        target = jnp.where(parent < 0, slots_one + 1, parent)
        sums = jax.ops.segment_sum(contrib, target, slots_one + 2)
        return sums[:slots_one], sums[slots_one + 1]

    owned, carried = lax.map(level_leaves, jnp.arange(n_dev, dtype=jnp.int32))
    live = jnp.sum((parents_one != slots_two).astype(jnp.int32), axis=1)
    signature_one = attach(owned, carried, live - 1)

    def level_boxes(inputs):
        field, parent, octant = inputs
        contrib = upsample_shift(wrap_pad(field), interp_two, octant, cos_two, sin_two)
        target = jnp.where(parent < 0, slots_two + 1, parent)
        sums = jax.ops.segment_sum(contrib, target, slots_two + 2)
        return sums[:slots_two], sums[slots_two + 1]

    owned_two, carried_two = lax.map(level_boxes, (signature_one, parents_one, octants_one))
    last_two = jnp.max(jnp.where(parents_one < slots_two, parents_one, -1), axis=1)
    signature_two = attach(owned_two, carried_two, last_two)
    return (signature_one.reshape(n_dev * slots_one, 2, signature_one.shape[-1]),
            signature_two.reshape(n_dev * slots_two, 2, signature_two.shape[-1]))
```

```python
import jax
import jax.numpy as jnp
from jax import lax
from jax.experimental import pallas as pl
from jax.experimental.pallas import tpu as pltpu
from jax.sharding import PartitionSpec as P

BF = jnp.bfloat16
F32 = jnp.float32

NCO = 625
KP = 640
PIECE = 688
CHUNK = 384
LROWS = 400
ROWS = 104
CARRY = 97


def grid_pairs(by, second):
    pairs = []
    for b in range(16):
        for x in range(4):
            for y in range(4):
                along_x = (b % 2 == 0) != second
                to = ((x + by) % 4, y) if along_x else (x, (y + by) % 4)
                pairs.append((b * 16 + 4 * x + y, b * 16 + 4 * to[0] + to[1]))
    return pairs


def shifted(array, by, second):
    return lax.ppermute(array, ("box", "angle"), grid_pairs(by, second))


def partner(array):
    return lax.ppermute(array, "box", [(i, i ^ 1) for i in range(16)])


def split(x):
    high = lax.reduce_precision(x, 8, 7)
    return high.astype(BF), (x - high).astype(BF)


def gather_pieces(piece):
    half = PIECE // 2
    left = shifted(piece, 1, False)
    right = shifted(piece, -1, False)
    top = shifted(left[:half], 1, False)
    bottom = shifted(right[half:], -1, False)
    stack = jnp.stack([piece, right, jnp.concatenate([top, bottom], axis=0), left])
    left2 = shifted(stack, 1, True)
    right2 = shifted(stack, -1, True)
    top2 = shifted(left2[:2], 1, True)
    bottom2 = shifted(right2[2:], -1, True)
    return [stack, right2, top2, bottom2, left2]


def leaf_kernel(table, s0, s1, s2, s3, s4, t0, t1, t2, t3, t4, lhs_r, lhs_i, octs, sums, out, w, x):
    for base, group in ((0, (s0, s1, s2, s3, s4)), (16, (t0, t1, t2, t3, t4))):
        n = 0
        for ref in group:
            for k in range(ref.shape[0]):
                w[table[base + n]] = ref[k]
                n += 1

    def product(p, _):
        wr = jnp.concatenate([w[2 * p, :KP, :], w[2 * p + 1, :KP, :]], axis=1)
        wi = jnp.concatenate([w[16 + 2 * p, :KP, :], w[17 + 2 * p, :KP, :]], axis=1)
        acc = jnp.dot(lhs_r[...], wr, preferred_element_type=F32)
        acc = acc + jnp.dot(lhs_i[...], wi, preferred_element_type=F32)
        acc = acc.astype(BF)
        x[2 * p] = acc[:, :128]
        x[2 * p + 1] = acc[:, 128:]
        return 0

    lax.fori_loop(0, 8, product, 0)
    x[16] = x[0]

    rows = lax.broadcasted_iota(jnp.int32, (256, 256), 0)
    cols = lax.broadcasted_iota(jnp.int32, (256, 256), 1)
    tap = rows - 63 - cols // 2
    row8 = lax.broadcasted_iota(jnp.int32, (8, 128), 0)
    sel_r = lax.broadcasted_iota(jnp.int32, (8, 512), 0)
    sel_c = lax.broadcasted_iota(jnp.int32, (8, 512), 1)
    pick_a = ((sel_r == 2) & (sel_c == 127)) | ((sel_r == 3) & (sel_c == 383))
    pick_b = (
        ((sel_r == 4) & (sel_c == 128))
        | ((sel_r == 5) & (sel_c == 129))
        | ((sel_r == 6) & (sel_c == 384))
        | ((sel_r == 7) & (sel_c == 385))
    )
    pick_a = jnp.where(pick_a, 1.0, 0.0).astype(BF)
    pick_b = jnp.where(pick_b, 1.0, 0.0).astype(BF)

    def window(q, _):
        nq = lax.rem(q + 1, 16)

        def banded(base):
            here = w[base + q, 672:688, :].astype(F32)
            there = w[base + nq, 672:688, :].astype(F32)
            full = jnp.zeros((256, 256), F32)
            for t in range(4):
                row = jnp.concatenate([here[4 + t : 5 + t], there[t : t + 1]], axis=1)
                full = jnp.where(tap == t, row, full)
            return full.astype(BF)

        def phases(base):
            both = jnp.concatenate([w[base + q, 656:672, :], w[base + nq, 640:656, :]], axis=1)
            return jnp.dot(octs[...], both, preferred_element_type=F32)

        src = jnp.concatenate([x[q], x[q + 1]], axis=1)
        y = jnp.dot(src, banded(0), preferred_element_type=F32)
        y = y + jnp.dot(src, banded(16), preferred_element_type=F32)
        cos = phases(0)
        sin = phases(16)
        yr = y[:LROWS]
        yi = y[LROWS:]
        z = jnp.concatenate([yr * cos - yi * sin, yr * sin + yi * cos], axis=1)
        high = z.astype(BF)
        low = (z - high.astype(F32)).astype(BF)
        part = jnp.dot(sums[...], high, preferred_element_type=F32)
        part = part + jnp.dot(sums[...], low, preferred_element_type=F32)
        part = part.astype(BF)
        nt = (((1,), (1,)), ((), ()))
        pad = jnp.zeros((8, 24), F32)
        edge_a = jnp.concatenate([lax.dot_general(pick_a, part, nt, preferred_element_type=F32), pad], axis=1)
        edge_b = jnp.concatenate([lax.dot_general(pick_b, part, nt, preferred_element_type=F32), pad], axis=1)
        out[q, :, 128:256] = part[:, :128]
        out[q, :, 384:512] = part[:, 256:384]
        out[nq, :, 0:128] = part[:, 128:256]
        out[nq, :, 256:384] = part[:, 384:512]
        last = part[96:104].astype(F32)
        out[nq, 96:104, 0:128] = jnp.where(row8 < 2, last[:, 128:256], edge_a).astype(BF)
        out[q, 96:104, 128:256] = jnp.where(row8 < 2, last[:, :128], edge_b).astype(BF)
        return 0

    lax.fori_loop(0, 16, window, 0)


def upper_kernel(recv, target, u_high, u_low, uh_re, uh_im, octs, cos_t, sin_t, sums, out1, out2, carry, acc):
    slot = lax.broadcasted_iota(jnp.int32, (768, ROWS), 0)
    nt = (((1,), (1,)), ((), ()))
    tn = (((0,), (0,)), ((), ()))
    row8 = lax.broadcasted_iota(jnp.int32, (8, ROWS), 0)
    acc[...] = jnp.zeros((768, 512), F32)

    def source(a, edge):
        onehot = jnp.where(slot == target[pl.ds(a, 1), :], 1.0, 0.0).astype(BF)
        acc[...] += jnp.dot(onehot, recv[a], preferred_element_type=F32)
        left = recv[a, 96:104, 0:ROWS].astype(F32)
        right = recv[a, 96:104, 128 : 128 + ROWS].astype(F32)
        rows = jnp.where(row8 < 2, 0.0, jnp.where(row8 < 4, left, right)).astype(BF)
        return edge + lax.dot_general(rows, onehot, nt, preferred_element_type=F32)

    edge = lax.fori_loop(0, 16, source, jnp.zeros((8, 768), F32))
    sig = acc[...]
    for part in range(2):
        for tile in range(2):
            lanes = slice(256 * part + 128 * tile, 256 * part + 128 * tile + 128)
            out1[pl.ds(2 * tile + part, 768, stride=4), :] = sig[:, lanes]
    x = sig.astype(BF)
    halo = jnp.concatenate([edge, edge], axis=0).astype(BF)

    def upsampled(part, extra):
        src = x[:, 256 * part : 256 * part + 256]
        y = jnp.dot(src, u_high[...], preferred_element_type=F32)
        y = y + jnp.dot(src, u_low[...], preferred_element_type=F32)
        return y + lax.dot_general(halo, extra[...], tn, preferred_element_type=F32)

    yr = upsampled(0, uh_re)
    yi = upsampled(1, uh_im)
    cos = jnp.dot(octs[...], cos_t[...], preferred_element_type=F32)
    sin = jnp.dot(octs[...], sin_t[...], preferred_element_type=F32)
    for part in range(2):
        z = yr * cos - yi * sin if part == 0 else yr * sin + yi * cos
        high = z.astype(BF)
        low = (z - high.astype(F32)).astype(BF)
        total = jnp.dot(sums[...], high, preferred_element_type=F32)
        total = total + jnp.dot(sums[...], low, preferred_element_type=F32)
        for tile in range(4):
            out2[pl.ds(2 * tile + part, 96, stride=8), :] = total[:96, 128 * tile : 128 * tile + 128]
        carry[:, 512 * part : 512 * part + 512] = total[96:104]


def vmem():
    return pl.BlockSpec(memory_space=pltpu.VMEM)


def body(
    coefficients,
    plane_map,
    leaf_parent,
    leaf_octant,
    box_parent,
    box_octant,
    interp_one,
    phase_one,
    interp_two,
    phase_two,
):
    place = lax.axis_index("angle")
    box = lax.axis_index("box")
    core = box % 2

    def halves(table):
        high, low = split(table)
        both = jnp.concatenate([high, low], axis=0)
        return jnp.concatenate([both[:, :128], both[:, 128:]], axis=0)

    w_high, w_low = split(interp_one)
    fold = lambda t: jnp.concatenate([t[:, :128], t[:, 128:], jnp.zeros((8, 128), BF)], axis=0)
    first = core == 0
    trig = halves(jnp.where(first, jnp.cos(phase_one), jnp.sin(phase_one)))
    weights = fold(jnp.where(first, w_high, w_low))
    piece = jnp.concatenate(
        [jnp.where(first, plane_map[0], plane_map[1]), jnp.zeros((KP - NCO, 128), BF), trig, weights], axis=0
    )
    mine = gather_pieces(piece)
    theirs = [partner(m) for m in mine]

    steps = jnp.arange(16, dtype=jnp.int32)
    order = jnp.concatenate([steps[:8], steps[8:12], steps[12:]])
    ahead = order % 4
    across = order // 4
    px, py = place // 4, place % 4

    def table_of(c):
        as_x = 4 * ((px + ahead) % 4) + (py + across) % 4
        as_y = 4 * ((px + across) % 4) + (py + ahead) % 4
        return 16 * c + jnp.where(c == 0, as_x, as_y)

    table = jnp.concatenate([table_of(core), table_of(1 - core)]).astype(jnp.int32)

    rows = jnp.transpose(coefficients, (0, 2, 1))
    lead_flag = jnp.where(leaf_parent[:8] < 0, 1.0, 0.0).astype(BF)
    lead_oct = leaf_octant[:8].astype(BF)
    note = jnp.concatenate([lead_flag[:, None], lead_oct[:, None], jnp.zeros((8, KP - NCO - 2), BF)], axis=1)
    lead = jnp.concatenate([rows[:, :8], jnp.stack([note, jnp.zeros_like(note)])], axis=2)
    lead = lax.ppermute(lead, ("box", "angle"), [(16 * (b + 1), 16 * b) for b in range(15)])
    lead_flag = lead[0, :, NCO]
    lead_oct = lead[0, :, NCO + 1].astype(jnp.int32)
    lead = jnp.pad(lead[:, :, :NCO], ((0, 0), (0, LROWS - CHUNK - 8), (0, KP - NCO)))
    rows = jnp.concatenate([jnp.pad(rows, ((0, 0), (0, 0), (0, KP - NCO))), lead], axis=1)
    lhs_r = jnp.concatenate([rows[0], rows[1]], axis=0)
    lhs_i = jnp.concatenate([-rows[1], rows[0]], axis=0)

    slots_one = box_parent.shape[0]
    slots_two = slots_one // 8
    starts = jnp.maximum(leaf_parent[::CHUNK], 0)
    parent = lax.dynamic_slice_in_dim(leaf_parent, place * CHUNK, CHUNK)
    octant = lax.dynamic_slice_in_dim(leaf_octant, place * CHUNK, CHUNK)
    live = (parent >= 0) & (parent < slots_one)
    target = jnp.where(live, parent - jnp.maximum(parent[0], 0), -1)
    none = jnp.full((8,), -1, jnp.int32)
    target = jnp.concatenate([target, jnp.where(lead_flag > 0.5, CARRY, -1), none])
    octant = jnp.concatenate([octant, lead_oct, none])
    sums = (jnp.arange(ROWS, dtype=jnp.int32)[:, None] == target[None, :]).astype(BF)
    octs = (octant[:, None] == jnp.arange(16, dtype=jnp.int32)[None, :] % 8).astype(BF)

    payload = pl.pallas_call(
        leaf_kernel,
        out_shape=jax.ShapeDtypeStruct((16, ROWS, 512), BF),
        in_specs=[pl.BlockSpec(memory_space=pltpu.SMEM)] + [vmem()] * 14,
        out_specs=vmem(),
        scratch_shapes=[pltpu.VMEM((32, PIECE, 128), BF), pltpu.VMEM((17, 2 * LROWS, 128), BF)],
        compiler_params=pltpu.CompilerParams(vmem_limit_bytes=56 << 20),
        name="leaf",
    )(table, *mine, *theirs, lhs_r, lhs_i, octs, sums)

    recv = lax.all_to_all(payload, "angle", split_axis=0, concat_axis=0, tiled=True)

    live_count = jnp.sum((box_parent != slots_two).astype(jnp.int32))
    row = jnp.arange(ROWS, dtype=jnp.int32)[None, :]
    slot = jnp.where(row < CARRY, starts[:, None] + row, -1)
    first_row = jnp.arange(16, dtype=jnp.int32)[:, None] == 0
    slot = jnp.where((row == CARRY) & first_row, live_count - 1, slot)

    col = jnp.arange(512, dtype=jnp.int32)[None, :] // 2

    def banded(sample):
        tap = sample[:, None] - col + 1
        full = jnp.zeros((sample.shape[0], 512), F32)
        for t in range(4):
            full = jnp.where(tap == t, interp_two[t][None, :], full)
        return split(full)

    u_high, u_low = banded(jnp.arange(256, dtype=jnp.int32))
    off = -1000
    re_high, re_low = banded(jnp.array([off, off, -1, off, 256, 257, off, off], jnp.int32))
    im_high, im_low = banded(jnp.array([off, off, off, -1, off, off, 256, 257], jnp.int32))
    cos_t = jnp.concatenate(split(jnp.cos(phase_two)), axis=0)
    sin_t = jnp.concatenate(split(jnp.sin(phase_two)), axis=0)
    octs_two = (box_octant[:, None] == jnp.arange(16, dtype=jnp.int32)[None, :] % 8).astype(BF)
    target_two = jnp.where(box_parent < 0, slots_two, jnp.where(box_parent < slots_two, box_parent, -1))
    sums_two = (jnp.arange(104, dtype=jnp.int32)[:, None] == target_two[None, :]).astype(BF)

    out1, out2, carry = pl.pallas_call(
        upper_kernel,
        out_shape=(
            jax.ShapeDtypeStruct((3072, 128), F32),
            jax.ShapeDtypeStruct((768, 128), F32),
            jax.ShapeDtypeStruct((8, 1024), F32),
        ),
        in_specs=[vmem()] * 10,
        out_specs=(vmem(), vmem(), vmem()),
        scratch_shapes=[pltpu.VMEM((768, 512), F32)],
        compiler_params=pltpu.CompilerParams(vmem_limit_bytes=56 << 20),
        name="upper",
    )(
        recv,
        slot,
        u_high,
        u_low,
        jnp.concatenate([re_high, re_low], axis=0),
        jnp.concatenate([im_high, im_low], axis=0),
        octs_two,
        cos_t,
        sin_t,
        sums_two,
    )
    signature_one = out1.reshape(768, 2, 2, 128).transpose(0, 2, 1, 3).reshape(768, 2, 256)
    own_two = out2.reshape(96, 4, 2, 128).transpose(0, 2, 1, 3).reshape(96, 2, 512)
    incoming = lax.ppermute(carry[:1], "box", [(i + 1, i) for i in range(15)]).reshape(1, 2, 512)
    last_two = jnp.max(jnp.where(box_parent < slots_two, box_parent, -1))
    chosen = (jnp.arange(slots_two, dtype=jnp.int32) == last_two).astype(F32)
    signature_two = own_two + chosen[:, None, None] * incoming
    return (signature_one, signature_two)


def solution(mesh):
    in_specs = (
        P(None, None, ("box", "angle")),
        P(None, None, "angle"),
        P("box"),
        P("box"),
        P("box"),
        P("box"),
        P(None, "angle"),
        P(None, "angle"),
        P(None, "angle"),
        P(None, "angle"),
    )
    out_specs = (P("box", None, "angle"), P("box", None, "angle"))
    return jax.shard_map(body, mesh=mesh, in_specs=in_specs, out_specs=out_specs, check_vma=False)
```

```python
import jax
import jax.numpy as jnp
from jax import lax
from jax.experimental import pallas as pl
from jax.experimental.pallas import tpu as pltpu
from jax.sharding import PartitionSpec as P

BF = jnp.bfloat16
F32 = jnp.float32

NCO = 625
KP = 640
PIECE = 688
CHUNK = 384
LROWS = 400
ROWS = 104
CARRY = 97


def grid_pairs(by, second):
    pairs = []
    for b in range(16):
        for x in range(4):
            for y in range(4):
                along_x = (b % 2 == 0) != second
                to = ((x + by) % 4, y) if along_x else (x, (y + by) % 4)
                pairs.append((b * 16 + 4 * x + y, b * 16 + 4 * to[0] + to[1]))
    return pairs


def shifted(array, by, second):
    return lax.ppermute(array, ("box", "angle"), grid_pairs(by, second))


def partner(array):
    return lax.ppermute(array, "box", [(i, i ^ 1) for i in range(16)])


def split(x):
    high = lax.reduce_precision(x, 8, 7)
    return high.astype(BF), (x - high).astype(BF)


def gather_pieces(piece):
    left = shifted(piece, 1, False)
    right = shifted(piece, -1, False)
    across = shifted(piece, 2, False)
    stack = jnp.stack([piece, right, across, left])
    left2 = shifted(stack, 1, True)
    right2 = shifted(stack, -1, True)
    top2 = shifted(left2[:2], 1, True)
    bottom2 = shifted(right2[2:], -1, True)
    return [stack, right2, top2, bottom2, left2]


def piece_kernel(core, plane, weights, phase, out):
    c = core[0]
    out[0:KP] = jnp.concatenate([plane[c], jnp.zeros((KP - NCO, 128), BF)], axis=0)
    angle = phase[...]
    trig = jnp.where(c == 0, jnp.cos(angle), jnp.sin(angle))
    high = trig.astype(BF)
    low = (trig - high.astype(F32)).astype(BF)
    for h in range(2):
        lanes = slice(128 * h, 128 * h + 128)
        out[KP + 16 * h : KP + 16 * h + 16] = jnp.concatenate([high[:, lanes], low[:, lanes]], axis=0)
    value = weights[...]
    high = value.astype(BF).astype(F32)
    value = jnp.where(c == 0, high, value - high)
    value = jnp.concatenate([value[:, :128], value[:, 128:], jnp.zeros((8, 128), F32)], axis=0)
    out[KP + 32 : KP + 48] = value.astype(BF)


def leaf_kernel(table, s0, s1, s2, s3, s4, t0, t1, t2, t3, t4, lhs, octs, sums, out, w, x, edge):
    for base, group in ((0, (s0, s1, s2, s3, s4)), (16, (t0, t1, t2, t3, t4))):
        n = 0
        for ref in group:
            for k in range(ref.shape[0]):
                w[table[base + n]] = ref[k]
                n += 1

    def product(p, _):
        wr = jnp.concatenate([w[2 * p, :KP, :], w[2 * p + 1, :KP, :]], axis=1)
        wi = jnp.concatenate([w[16 + 2 * p, :KP, :], w[17 + 2 * p, :KP, :]], axis=1)
        acc = jnp.dot(lhs[...], jnp.concatenate([wr, wi], axis=0), preferred_element_type=F32)
        acc = acc.astype(BF)
        x[2 * p + 1] = acc[:, :128]
        x[2 * p + 2] = acc[:, 128:]
        return 0

    lax.fori_loop(0, 8, product, 0)
    x[0] = x[16]
    x[17] = x[1]

    rows = lax.broadcasted_iota(jnp.int32, (256, 256), 0)
    cols = lax.broadcasted_iota(jnp.int32, (256, 256), 1)
    edge_row = (rows == 128) | (rows == 129) | (rows == 255)
    sample = jnp.where(rows < 128, rows, jnp.where(rows < 130, rows, jnp.where(rows == 255, -1, rows - 128)))
    tap = sample + 1 - cols // 2
    high_row = (rows < 128) | edge_row
    lane = lax.broadcasted_iota(jnp.int32, (2 * LROWS, 128), 1)
    row8 = lax.broadcasted_iota(jnp.int32, (8, 128), 0)
    sel_r = lax.broadcasted_iota(jnp.int32, (16, 512), 0)
    sel_c = lax.broadcasted_iota(jnp.int32, (16, 512), 1)
    pick = ((sel_r == 2) & (sel_c == 255)) | ((sel_r == 3) & (sel_c == 511))
    for r, c in ((12, 0), (13, 1), (14, 256), (15, 257)):
        pick = pick | ((sel_r == r) & (sel_c == c))
    pick = jnp.where(pick, 1.0, 0.0).astype(BF)

    def window(q, _):
        def row_of(base, t):
            both = w[base + q, 672:688, :].astype(F32)
            return jnp.concatenate([both[t : t + 1], both[4 + t : 5 + t]], axis=1)

        band = jnp.zeros((256, 256), F32)
        for t in range(4):
            band = jnp.where(tap == t, jnp.where(high_row, row_of(0, t), row_of(16, t)), band)

        def phases(base):
            both = jnp.concatenate([w[base + q, 640:656, :], w[base + q, 656:672, :]], axis=1)
            return jnp.dot(octs[...], both, preferred_element_type=F32)

        own = x[q + 1]
        side = jnp.where(lane < 2, x[q + 2], jnp.where(lane == 127, x[q], own))
        y = jnp.dot(jnp.concatenate([own, side], axis=1), band.astype(BF), preferred_element_type=F32)
        cos = phases(0)
        sin = phases(16)
        yr = y[:LROWS]
        yi = y[LROWS:]
        z = jnp.concatenate([yr * cos - yi * sin, yr * sin + yi * cos], axis=1)
        high = z.astype(BF)
        low = (z - high.astype(F32)).astype(BF)
        part = jnp.dot(sums[...], high, preferred_element_type=F32)
        part = part + jnp.dot(sums[...], low, preferred_element_type=F32)
        part = part.astype(BF)
        out[q] = part
        ends = lax.dot_general(pick, part, (((1,), (1,)), ((), ())), preferred_element_type=F32)
        ends = jnp.concatenate([ends, jnp.zeros((16, 24), F32)], axis=1)
        edge[0, lax.rem(q + 1, 16)] = ends[:8]
        edge[1, lax.rem(q + 15, 16)] = ends[8:]
        return 0

    lax.fori_loop(0, 16, window, 0)

    def finish(q, _):
        last = out[q, 96:104, 0:128].astype(F32)
        out[q, 96:104, 0:128] = jnp.where(row8 < 2, last, edge[0, q] + edge[1, q]).astype(BF)
        return 0

    lax.fori_loop(0, 16, finish, 0)


def upper_kernel(recv, target, u_high, u_low, uh_re, uh_im, octs, cos_t, sin_t, sums, out1, out2, carry):
    slot = lax.broadcasted_iota(jnp.int32, (768, 16 * ROWS), 0)
    nt = (((1,), (1,)), ((), ()))
    tn = (((0,), (0,)), ((), ()))
    onehot = jnp.where(slot == target[...], 1.0, 0.0).astype(BF)
    sig = jnp.dot(onehot, recv[...], preferred_element_type=F32)
    ends = [recv[ROWS * a + 96 : ROWS * a + 104, 0:ROWS].astype(F32) for a in range(16)]
    ends = jnp.concatenate(ends, axis=1)
    ends = jnp.where(lax.broadcasted_iota(jnp.int32, (8, 16 * ROWS), 0) < 2, 0.0, ends).astype(BF)
    edge = lax.dot_general(ends, onehot, nt, preferred_element_type=F32)
    for part in range(2):
        for tile in range(2):
            lanes = slice(256 * part + 128 * tile, 256 * part + 128 * tile + 128)
            out1[pl.ds(2 * tile + part, 768, stride=4), :] = sig[:, lanes]
    x = sig.astype(BF)
    halo = jnp.concatenate([edge, edge], axis=0).astype(BF)

    def upsampled(part, extra):
        src = x[:, 256 * part : 256 * part + 256]
        y = jnp.dot(src, u_high[...], preferred_element_type=F32)
        y = y + jnp.dot(src, u_low[...], preferred_element_type=F32)
        return y + lax.dot_general(halo, extra[...], tn, preferred_element_type=F32)

    yr = upsampled(0, uh_re)
    yi = upsampled(1, uh_im)
    cos = jnp.dot(octs[...], cos_t[...], preferred_element_type=F32)
    sin = jnp.dot(octs[...], sin_t[...], preferred_element_type=F32)
    for part in range(2):
        z = yr * cos - yi * sin if part == 0 else yr * sin + yi * cos
        high = z.astype(BF)
        low = (z - high.astype(F32)).astype(BF)
        total = jnp.dot(sums[...], high, preferred_element_type=F32)
        total = total + jnp.dot(sums[...], low, preferred_element_type=F32)
        for tile in range(4):
            out2[pl.ds(2 * tile + part, 96, stride=8), :] = total[:96, 128 * tile : 128 * tile + 128]
            carry[2 * tile + part : 2 * tile + part + 1, :] = total[96:97, 128 * tile : 128 * tile + 128]


def vmem():
    return pl.BlockSpec(memory_space=pltpu.VMEM)


def body(
    coefficients,
    plane_map,
    leaf_parent,
    leaf_octant,
    box_parent,
    box_octant,
    interp_one,
    phase_one,
    interp_two,
    phase_two,
):
    place = lax.axis_index("angle")
    box = lax.axis_index("box")
    core = box % 2

    piece = pl.pallas_call(
        piece_kernel,
        out_shape=jax.ShapeDtypeStruct((PIECE, 128), BF),
        in_specs=[pl.BlockSpec(memory_space=pltpu.SMEM)] + [vmem()] * 3,
        out_specs=vmem(),
        compiler_params=pltpu.CompilerParams(vmem_limit_bytes=8 << 20),
        name="piece",
    )(core.reshape(1), plane_map, interp_one, phase_one)
    mine = gather_pieces(piece)
    theirs = [partner(m) for m in mine]

    steps = jnp.arange(16, dtype=jnp.int32)
    order = jnp.concatenate([steps[:8], steps[8:12], steps[12:]])
    ahead = order % 4
    across = order // 4
    px, py = place // 4, place % 4

    def table_of(c):
        as_x = 4 * ((px + ahead) % 4) + (py + across) % 4
        as_y = 4 * ((px + across) % 4) + (py + ahead) % 4
        return 16 * c + jnp.where(c == 0, as_x, as_y)

    table = jnp.concatenate([table_of(core), table_of(1 - core)]).astype(jnp.int32)

    coefficients, mine[0] = lax.optimization_barrier((coefficients, mine[0]))
    rows = jnp.transpose(coefficients, (0, 2, 1))
    lead_flag = jnp.where(leaf_parent[:8] < 0, 1.0, 0.0).astype(BF)
    lead_oct = leaf_octant[:8].astype(BF)
    note = jnp.concatenate([lead_flag[:, None], lead_oct[:, None], jnp.zeros((8, KP - NCO - 2), BF)], axis=1)
    lead = jnp.concatenate([rows[:, :8], jnp.stack([note, jnp.zeros_like(note)])], axis=2)
    lead = lax.ppermute(lead, ("box", "angle"), [(16 * (b + 1), 16 * b) for b in range(15)])
    lead_flag = lead[0, :, NCO]
    lead_oct = lead[0, :, NCO + 1].astype(jnp.int32)
    lead = jnp.pad(lead[:, :, :NCO], ((0, 0), (0, LROWS - CHUNK - 8), (0, KP - NCO)))
    rows = jnp.concatenate([jnp.pad(rows, ((0, 0), (0, 0), (0, KP - NCO))), lead], axis=1)
    lhs = jnp.concatenate(
        [jnp.concatenate([rows[0], rows[1]], axis=0), jnp.concatenate([-rows[1], rows[0]], axis=0)], axis=1
    )

    slots_one = box_parent.shape[0]
    slots_two = slots_one // 8
    starts = jnp.maximum(leaf_parent[::CHUNK], 0)
    parent = lax.dynamic_slice_in_dim(leaf_parent, place * CHUNK, CHUNK)
    octant = lax.dynamic_slice_in_dim(leaf_octant, place * CHUNK, CHUNK)
    live = (parent >= 0) & (parent < slots_one)
    target = jnp.where(live, parent - jnp.maximum(parent[0], 0), -1)
    none = jnp.full((8,), -1, jnp.int32)
    target = jnp.concatenate([target, jnp.where(lead_flag > 0.5, CARRY, -1), none])
    octant = jnp.concatenate([octant, lead_oct, none])
    sums = (jnp.arange(ROWS, dtype=jnp.int32)[:, None] == target[None, :]).astype(BF)
    octs = (octant[:, None] == jnp.arange(16, dtype=jnp.int32)[None, :] % 8).astype(BF)

    payload = pl.pallas_call(
        leaf_kernel,
        out_shape=jax.ShapeDtypeStruct((16, ROWS, 512), BF),
        in_specs=[pl.BlockSpec(memory_space=pltpu.SMEM)] + [vmem()] * 13,
        out_specs=vmem(),
        scratch_shapes=[pltpu.VMEM((32, PIECE, 128), BF), pltpu.VMEM((18, 2 * LROWS, 128), BF), pltpu.VMEM((2, 16, 8, 128), F32)],
        compiler_params=pltpu.CompilerParams(vmem_limit_bytes=28 << 20),
        name="leaf",
    )(table, *mine, *theirs, lhs, octs, sums)

    recv = lax.all_to_all(payload, "angle", split_axis=0, concat_axis=0, tiled=True)

    last_two = jnp.max(jnp.where(box_parent < slots_two, box_parent, -1))
    live_count = jnp.sum((box_parent != slots_two).astype(jnp.int32))
    row = jnp.arange(ROWS, dtype=jnp.int32)[None, :]
    slot = jnp.where(row < CARRY, starts[:, None] + row, -1)
    first_row = jnp.arange(16, dtype=jnp.int32)[:, None] == 0
    slot = jnp.where((row == CARRY) & first_row, live_count - 1, slot)

    col = jnp.arange(512, dtype=jnp.int32)[None, :] // 2

    def banded(sample):
        tap = sample[:, None] - col + 1
        full = jnp.zeros((sample.shape[0], 512), F32)
        for t in range(4):
            full = jnp.where(tap == t, interp_two[t][None, :], full)
        return split(full)

    u_high, u_low = banded(jnp.arange(256, dtype=jnp.int32))
    off = -1000
    re_high, re_low = banded(jnp.array([off, off, -1, off, 256, 257, off, off], jnp.int32))
    im_high, im_low = banded(jnp.array([off, off, off, -1, off, off, 256, 257], jnp.int32))
    cos_t = jnp.concatenate(split(jnp.cos(phase_two)), axis=0)
    sin_t = jnp.concatenate(split(jnp.sin(phase_two)), axis=0)
    octs_two = (box_octant[:, None] == jnp.arange(16, dtype=jnp.int32)[None, :] % 8).astype(BF)
    target_two = jnp.where(box_parent < 0, slots_two, jnp.where(box_parent < slots_two, box_parent, -1))
    sums_two = (jnp.arange(104, dtype=jnp.int32)[:, None] == target_two[None, :]).astype(BF)

    out1, out2, carry = pl.pallas_call(
        upper_kernel,
        out_shape=(
            jax.ShapeDtypeStruct((3072, 128), F32),
            jax.ShapeDtypeStruct((768, 128), F32),
            jax.ShapeDtypeStruct((8, 128), F32),
        ),
        in_specs=[vmem()] * 10,
        out_specs=(vmem(), vmem(), vmem()),
        compiler_params=pltpu.CompilerParams(vmem_limit_bytes=28 << 20),
        name="upper",
    )(
        recv.reshape(16 * ROWS, 512),
        slot.reshape(1, 16 * ROWS),
        u_high,
        u_low,
        jnp.concatenate([re_high, re_low], axis=0),
        jnp.concatenate([im_high, im_low], axis=0),
        octs_two,
        cos_t,
        sin_t,
        sums_two,
    )
    signature_one = out1.reshape(768, 2, 2, 128).transpose(0, 2, 1, 3).reshape(768, 2, 256)
    incoming = lax.ppermute(carry, "box", [(i + 1, i) for i in range(15)])
    incoming = jnp.where(last_two < 0, 0.0, incoming)
    at = 8 * jnp.maximum(last_two, 0)
    out2 = lax.dynamic_update_slice_in_dim(out2, lax.dynamic_slice_in_dim(out2, at, 8, 0) + incoming, at, 0)
    signature_two = out2.reshape(96, 4, 2, 128).transpose(0, 2, 1, 3).reshape(96, 2, 512)
    return (signature_one, signature_two)


def solution(mesh):
    in_specs = (
        P(None, None, ("box", "angle")),
        P(None, None, "angle"),
        P("box"),
        P("box"),
        P("box"),
        P("box"),
        P(None, "angle"),
        P(None, "angle"),
        P(None, "angle"),
        P(None, "angle"),
    )
    out_specs = (P("box", None, "angle"), P("box", None, "angle"))
    return jax.shard_map(body, mesh=mesh, in_specs=in_specs, out_specs=out_specs, check_vma=False)
```

```python
import jax
import jax.numpy as jnp
from jax import lax
from jax.experimental import pallas as pl
from jax.experimental.pallas import tpu as pltpu
from jax.sharding import PartitionSpec as P

BF = jnp.bfloat16
F32 = jnp.float32

NCO = 625
KP = 640
PIECE = 688
CHUNK = 384
LROWS = 400
ROWS = 104
CARRY = 97


def grid_pairs(by, second):
    pairs = []
    for b in range(16):
        for x in range(4):
            for y in range(4):
                along_x = (b % 2 == 0) != second
                to = ((x + by) % 4, y) if along_x else (x, (y + by) % 4)
                pairs.append((b * 16 + 4 * x + y, b * 16 + 4 * to[0] + to[1]))
    return pairs


def shifted(array, by, second):
    return lax.ppermute(array, ("box", "angle"), grid_pairs(by, second))


def partner(array):
    return lax.ppermute(array, "box", [(i, i ^ 1) for i in range(16)])


def split(x):
    high = lax.reduce_precision(x, 8, 7)
    return high.astype(BF), (x - high).astype(BF)


def gather_pieces(piece):
    left = shifted(piece, 1, False)
    right = shifted(piece, -1, False)
    across = shifted(piece, 2, False)
    stack = jnp.stack([piece, right, across, left])
    return [stack, shifted(stack, -1, True), shifted(stack, 2, True), shifted(stack, 1, True)]


def piece_kernel(core, plane, weights, phase, out):
    c = core[0]
    out[0:KP] = jnp.concatenate([plane[c], jnp.zeros((KP - NCO, 128), BF)], axis=0)
    angle = phase[...]
    trig = jnp.where(c == 0, jnp.cos(angle), jnp.sin(angle))
    high = trig.astype(BF)
    low = (trig - high.astype(F32)).astype(BF)
    for h in range(2):
        lanes = slice(128 * h, 128 * h + 128)
        out[KP + 16 * h : KP + 16 * h + 16] = jnp.concatenate([high[:, lanes], low[:, lanes]], axis=0)
    value = weights[...]
    high = value.astype(BF).astype(F32)
    value = jnp.where(c == 0, high, value - high)
    value = jnp.concatenate([value[:, :128], value[:, 128:], jnp.zeros((8, 128), F32)], axis=0)
    out[KP + 32 : KP + 48] = value.astype(BF)


def leaf_kernel(table, s0, s1, s2, s3, t0, t1, t2, t3, lhs, octs, sums, out, w, x, edge):
    for base, group in ((0, (s0, s1, s2, s3)), (16, (t0, t1, t2, t3))):
        n = 0
        for ref in group:
            for k in range(ref.shape[0]):
                w[table[base + n]] = ref[k]
                n += 1

    def product(p, _):
        wr = jnp.concatenate([w[2 * p, :KP, :], w[2 * p + 1, :KP, :]], axis=1)
        wi = jnp.concatenate([w[16 + 2 * p, :KP, :], w[17 + 2 * p, :KP, :]], axis=1)
        acc = jnp.dot(lhs[...], jnp.concatenate([wr, wi], axis=0), preferred_element_type=F32)
        acc = acc.astype(BF)
        x[2 * p + 1] = acc[:, :128]
        x[2 * p + 2] = acc[:, 128:]
        return 0

    lax.fori_loop(0, 8, product, 0, unroll=2)
    x[0] = x[16]
    x[17] = x[1]

    rows = lax.broadcasted_iota(jnp.int32, (256, 256), 0)
    cols = lax.broadcasted_iota(jnp.int32, (256, 256), 1)
    edge_row = (rows == 128) | (rows == 129) | (rows == 255)
    sample = jnp.where(rows < 128, rows, jnp.where(rows < 130, rows, jnp.where(rows == 255, -1, rows - 128)))
    tap = sample + 1 - cols // 2
    high_row = (rows < 128) | edge_row
    lane = lax.broadcasted_iota(jnp.int32, (2 * LROWS, 128), 1)
    row8 = lax.broadcasted_iota(jnp.int32, (8, 128), 0)
    sel_r = lax.broadcasted_iota(jnp.int32, (16, 512), 0)
    sel_c = lax.broadcasted_iota(jnp.int32, (16, 512), 1)
    pick = ((sel_r == 2) & (sel_c == 255)) | ((sel_r == 3) & (sel_c == 511))
    for r, c in ((12, 0), (13, 1), (14, 256), (15, 257)):
        pick = pick | ((sel_r == r) & (sel_c == c))
    pick = jnp.where(pick, 1.0, 0.0).astype(BF)

    def window(q, _):
        def row_of(base, t):
            both = w[base + q, 672:688, :].astype(F32)
            return jnp.concatenate([both[t : t + 1], both[4 + t : 5 + t]], axis=1)

        band = jnp.zeros((256, 256), F32)
        for t in range(4):
            band = jnp.where(tap == t, jnp.where(high_row, row_of(0, t), row_of(16, t)), band)

        def phases(base):
            both = jnp.concatenate([w[base + q, 640:656, :], w[base + q, 656:672, :]], axis=1)
            return jnp.dot(octs[...], both, preferred_element_type=F32)

        own = x[q + 1]
        side = jnp.where(lane < 2, x[q + 2], jnp.where(lane == 127, x[q], own))
        y = jnp.dot(jnp.concatenate([own, side], axis=1), band.astype(BF), preferred_element_type=F32)
        cos = phases(0)
        sin = phases(16)
        yr = y[:LROWS]
        yi = y[LROWS:]
        z = jnp.concatenate([yr * cos - yi * sin, yr * sin + yi * cos], axis=1)
        high = z.astype(BF)
        low = (z - high.astype(F32)).astype(BF)
        part = jnp.dot(sums[...], high, preferred_element_type=F32)
        part = part + jnp.dot(sums[...], low, preferred_element_type=F32)
        part = part.astype(BF)
        out[q] = part
        ends = lax.dot_general(pick, part, (((1,), (1,)), ((), ())), preferred_element_type=F32)
        ends = jnp.concatenate([ends, jnp.zeros((16, 24), F32)], axis=1)
        edge[0, lax.rem(q + 1, 16)] = ends[:8]
        edge[1, lax.rem(q + 15, 16)] = ends[8:]
        return 0

    lax.fori_loop(0, 16, window, 0, unroll=4)

    def finish(q, _):
        last = out[q, 96:104, 0:128].astype(F32)
        out[q, 96:104, 0:128] = jnp.where(row8 < 2, last, edge[0, q] + edge[1, q]).astype(BF)
        return 0

    lax.fori_loop(0, 16, finish, 0)


def received(rows, recv, target):
    slot = lax.broadcasted_iota(jnp.int32, (rows, 16 * ROWS), 0)
    onehot = jnp.where(slot == target[...], 1.0, 0.0).astype(BF)
    sig = jnp.dot(onehot, recv[...], preferred_element_type=F32)
    ends = [recv[ROWS * a + 96 : ROWS * a + 104, 0:ROWS].astype(F32) for a in range(16)]
    ends = jnp.concatenate(ends, axis=1)
    ends = jnp.where(lax.broadcasted_iota(jnp.int32, (8, 16 * ROWS), 0) < 2, 0.0, ends).astype(BF)
    edge = lax.dot_general(ends, onehot, (((1,), (1,)), ((), ())), preferred_element_type=F32)
    return sig, jnp.concatenate([edge, edge], axis=0).astype(BF)


def raised(sig, halo, u_high, u_low, extras, octs, cos_t, sin_t):
    x = sig.astype(BF)

    def upsampled(part):
        src = x[:, 256 * part : 256 * part + 256]
        y = jnp.dot(src, u_high[...], preferred_element_type=F32)
        y = y + jnp.dot(src, u_low[...], preferred_element_type=F32)
        return y + lax.dot_general(halo, extras[part][...], (((0,), (0,)), ((), ())), preferred_element_type=F32)

    yr = upsampled(0)
    yi = upsampled(1)
    cos = jnp.dot(octs, cos_t[...], preferred_element_type=F32)
    sin = jnp.dot(octs, sin_t[...], preferred_element_type=F32)
    return yr * cos - yi * sin, yr * sin + yi * cos


def lead_kernel(recv, target, u_high, u_low, uh_re, uh_im, octs, cos_t, sin_t, mask, carry):
    sig, halo = received(16, recv, target)
    parts = raised(sig, halo, u_high, u_low, (uh_re, uh_im), octs[0:16], cos_t, sin_t)
    for part in range(2):
        total = jnp.sum(jnp.where(mask[...] > 0.5, parts[part], 0.0), axis=0, keepdims=True)
        for tile in range(4):
            carry[2 * tile + part : 2 * tile + part + 1, :] = total[:, 128 * tile : 128 * tile + 128]


def upper_kernel(recv, target, u_high, u_low, uh_re, uh_im, octs, cos_t, sin_t, sums, out1, out2):
    sig, halo = received(768, recv, target)
    for part in range(2):
        for tile in range(2):
            lanes = slice(256 * part + 128 * tile, 256 * part + 128 * tile + 128)
            out1[pl.ds(2 * tile + part, 768, stride=4), :] = sig[:, lanes]
    parts = raised(sig, halo, u_high, u_low, (uh_re, uh_im), octs[...], cos_t, sin_t)
    for part in range(2):
        z = parts[part]
        high = z.astype(BF)
        low = (z - high.astype(F32)).astype(BF)
        total = jnp.dot(sums[...], high, preferred_element_type=F32)
        total = total + jnp.dot(sums[...], low, preferred_element_type=F32)
        for tile in range(4):
            out2[pl.ds(2 * tile + part, 96, stride=8), :] = total[:, 128 * tile : 128 * tile + 128]


def vmem():
    return pl.BlockSpec(memory_space=pltpu.VMEM)


def body(
    coefficients,
    plane_map,
    leaf_parent,
    leaf_octant,
    box_parent,
    box_octant,
    interp_one,
    phase_one,
    interp_two,
    phase_two,
):
    place = lax.axis_index("angle")
    box = lax.axis_index("box")
    core = box % 2

    piece = pl.pallas_call(
        piece_kernel,
        out_shape=jax.ShapeDtypeStruct((PIECE, 128), BF),
        in_specs=[pl.BlockSpec(memory_space=pltpu.SMEM)] + [vmem()] * 3,
        out_specs=vmem(),
        compiler_params=pltpu.CompilerParams(vmem_limit_bytes=8 << 20),
        name="piece",
    )(core.reshape(1), plane_map, interp_one, phase_one)
    mine = gather_pieces(piece)
    theirs = [partner(m) for m in mine]

    steps = jnp.arange(16, dtype=jnp.int32)
    ahead = steps % 4
    across = steps // 4
    px, py = place // 4, place % 4

    def table_of(c):
        as_x = 4 * ((px + ahead) % 4) + (py + across) % 4
        as_y = 4 * ((px + across) % 4) + (py + ahead) % 4
        return 16 * c + jnp.where(c == 0, as_x, as_y)

    table = jnp.concatenate([table_of(core), table_of(1 - core)]).astype(jnp.int32)

    lead_flag = jnp.where(leaf_parent[:8] < 0, 1.0, 0.0).astype(BF)
    lead_oct = leaf_octant[:8].astype(BF)
    note = jnp.concatenate([lead_flag[:, None], lead_oct[:, None], jnp.zeros((8, KP - NCO - 2), BF)], axis=1)
    lead = jnp.transpose(coefficients[:, :, :8], (0, 2, 1))
    lead = jnp.concatenate([lead, jnp.stack([note, jnp.zeros_like(note)])], axis=2)
    lead = lax.ppermute(lead, ("box", "angle"), [(16 * (b + 1), 16 * b) for b in range(15)])
    coefficients, lead, leaf_parent, leaf_octant, box_parent, mine[0] = lax.optimization_barrier(
        (coefficients, lead, leaf_parent, leaf_octant, box_parent, mine[0])
    )
    slots_one = box_parent.shape[0]
    slots_two = slots_one // 8
    starts = jnp.maximum(leaf_parent[::CHUNK], 0)
    last_two = jnp.max(jnp.where(box_parent < slots_two, box_parent, -1))
    live_count = jnp.sum((box_parent != slots_two).astype(jnp.int32))
    rows = jnp.transpose(coefficients, (0, 2, 1))
    lead_flag = lead[0, :, NCO]
    lead_oct = lead[0, :, NCO + 1].astype(jnp.int32)
    lead = jnp.pad(lead[:, :, :NCO], ((0, 0), (0, LROWS - CHUNK - 8), (0, KP - NCO)))
    rows = jnp.concatenate([jnp.pad(rows, ((0, 0), (0, 0), (0, KP - NCO))), lead], axis=1)
    lhs = jnp.concatenate(
        [jnp.concatenate([rows[0], rows[1]], axis=0), jnp.concatenate([-rows[1], rows[0]], axis=0)], axis=1
    )

    parent = lax.dynamic_slice_in_dim(leaf_parent, place * CHUNK, CHUNK)
    octant = lax.dynamic_slice_in_dim(leaf_octant, place * CHUNK, CHUNK)
    live = (parent >= 0) & (parent < slots_one)
    target = jnp.where(live, parent - jnp.maximum(parent[0], 0), -1)
    none = jnp.full((8,), -1, jnp.int32)
    target = jnp.concatenate([target, jnp.where(lead_flag > 0.5, CARRY, -1), none])
    octant = jnp.concatenate([octant, lead_oct, none])
    sums = (jnp.arange(ROWS, dtype=jnp.int32)[:, None] == target[None, :]).astype(BF)
    octs = (octant[:, None] == jnp.arange(16, dtype=jnp.int32)[None, :] % 8).astype(BF)

    payload = pl.pallas_call(
        leaf_kernel,
        out_shape=jax.ShapeDtypeStruct((16, ROWS, 512), BF),
        in_specs=[pl.BlockSpec(memory_space=pltpu.SMEM)] + [vmem()] * 11,
        out_specs=vmem(),
        scratch_shapes=[pltpu.VMEM((32, PIECE, 128), BF), pltpu.VMEM((18, 2 * LROWS, 128), BF), pltpu.VMEM((2, 16, 8, 128), F32)],
        compiler_params=pltpu.CompilerParams(vmem_limit_bytes=28 << 20),
        name="leaf",
    )(table, *mine, *theirs, lhs, octs, sums)

    box_parent, box_octant, interp_two, phase_two, payload = lax.optimization_barrier(
        (box_parent, box_octant, interp_two, phase_two, payload)
    )
    recv = lax.all_to_all(payload, "angle", split_axis=0, concat_axis=0, tiled=True)

    row = jnp.arange(ROWS, dtype=jnp.int32)[None, :]
    slot = jnp.where(row < CARRY, starts[:, None] + row, -1)
    first_row = jnp.arange(16, dtype=jnp.int32)[:, None] == 0
    slot = jnp.where((row == CARRY) & first_row, live_count - 1, slot)

    col = jnp.arange(512, dtype=jnp.int32)[None, :] // 2

    def banded(sample):
        tap = sample[:, None] - col + 1
        full = jnp.zeros((sample.shape[0], 512), F32)
        for t in range(4):
            full = jnp.where(tap == t, interp_two[t][None, :], full)
        return split(full)

    u_high, u_low = banded(jnp.arange(256, dtype=jnp.int32))
    off = -1000
    re_high, re_low = banded(jnp.array([off, off, -1, off, 256, 257, off, off], jnp.int32))
    im_high, im_low = banded(jnp.array([off, off, off, -1, off, off, 256, 257], jnp.int32))
    cos_t = jnp.concatenate(split(jnp.cos(phase_two)), axis=0)
    sin_t = jnp.concatenate(split(jnp.sin(phase_two)), axis=0)
    octs_two = (box_octant[:, None] == jnp.arange(16, dtype=jnp.int32)[None, :] % 8).astype(BF)
    sums_two = (jnp.arange(slots_two, dtype=jnp.int32)[:, None] == box_parent[None, :]).astype(BF)
    lead_mask = jnp.broadcast_to((box_parent[:16, None] < 0).astype(F32), (16, 512))

    operands = (
        recv.reshape(16 * ROWS, 512),
        slot.reshape(1, 16 * ROWS),
        u_high,
        u_low,
        jnp.concatenate([re_high, re_low], axis=0),
        jnp.concatenate([im_high, im_low], axis=0),
        octs_two,
        cos_t,
        sin_t,
    )
    carry = pl.pallas_call(
        lead_kernel,
        out_shape=jax.ShapeDtypeStruct((8, 128), F32),
        in_specs=[vmem()] * 10,
        out_specs=vmem(),
        compiler_params=pltpu.CompilerParams(vmem_limit_bytes=16 << 20),
        name="lead",
    )(*operands, lead_mask)
    incoming = lax.ppermute(carry, "box", [(i + 1, i) for i in range(15)])
    out1, out2 = pl.pallas_call(
        upper_kernel,
        out_shape=(jax.ShapeDtypeStruct((3072, 128), F32), jax.ShapeDtypeStruct((768, 128), F32)),
        in_specs=[vmem()] * 10,
        out_specs=(vmem(), vmem()),
        compiler_params=pltpu.CompilerParams(vmem_limit_bytes=28 << 20),
        name="upper",
    )(*operands, sums_two)
    signature_one = out1.reshape(768, 2, 2, 128).transpose(0, 2, 1, 3).reshape(768, 2, 256)
    incoming = jnp.where(last_two < 0, 0.0, incoming)
    at = 8 * jnp.maximum(last_two, 0)
    out2 = lax.dynamic_update_slice_in_dim(out2, lax.dynamic_slice_in_dim(out2, at, 8, 0) + incoming, at, 0)
    signature_two = out2.reshape(96, 4, 2, 128).transpose(0, 2, 1, 3).reshape(96, 2, 512)
    return (signature_one, signature_two)


def solution(mesh):
    in_specs = (
        P(None, None, ("box", "angle")),
        P(None, None, "angle"),
        P("box"),
        P("box"),
        P("box"),
        P("box"),
        P(None, "angle"),
        P(None, "angle"),
        P(None, "angle"),
        P(None, "angle"),
    )
    out_specs = (P("box", None, "angle"), P("box", None, "angle"))
    return jax.shard_map(body, mesh=mesh, in_specs=in_specs, out_specs=out_specs, check_vma=False)
```

```python
import jax
import jax.numpy as jnp
from jax import lax
from jax.experimental import pallas as pl
from jax.experimental.pallas import tpu as pltpu
from jax.sharding import PartitionSpec as P

BF = jnp.bfloat16
F32 = jnp.float32

NCO = 625
KP = 640
PIECE = 688
CHUNK = 384
LROWS = 400
ROWS = 104
CARRY = 97


def grid_pairs(by, second):
    pairs = []
    for b in range(16):
        for x in range(4):
            for y in range(4):
                along_x = (b % 2 == 0) != second
                to = ((x + by) % 4, y) if along_x else (x, (y + by) % 4)
                pairs.append((b * 16 + 4 * x + y, b * 16 + 4 * to[0] + to[1]))
    return pairs


def shifted(array, by, second):
    return lax.ppermute(array, ("box", "angle"), grid_pairs(by, second))


def partner(array):
    return lax.ppermute(array, "box", [(i, i ^ 1) for i in range(16)])


def split(x):
    high = lax.reduce_precision(x, 8, 7)
    return high.astype(BF), (x - high).astype(BF)


def gather_pieces(piece):
    left = shifted(piece, 1, False)
    right = shifted(piece, -1, False)
    across = shifted(piece, 2, False)
    stack = jnp.stack([piece, right, across, left])
    return [stack, shifted(stack, -1, True), shifted(stack, 2, True), shifted(stack, 1, True)]


def piece_kernel(core, plane, weights, phase, out):
    c = core[0]
    out[0:KP] = jnp.concatenate([plane[c], jnp.zeros((KP - NCO, 128), BF)], axis=0)
    angle = phase[...]
    trig = jnp.where(c == 0, jnp.cos(angle), jnp.sin(angle))
    high = trig.astype(BF)
    low = (trig - high.astype(F32)).astype(BF)
    for h in range(2):
        lanes = slice(128 * h, 128 * h + 128)
        out[KP + 16 * h : KP + 16 * h + 16] = jnp.concatenate([high[:, lanes], low[:, lanes]], axis=0)
    value = weights[...]
    high = value.astype(BF).astype(F32)
    value = jnp.where(c == 0, high, value - high)
    value = jnp.concatenate([value[:, :128], value[:, 128:], jnp.zeros((8, 128), F32)], axis=0)
    out[KP + 32 : KP + 48] = value.astype(BF)


def leaf_kernel(table, s0, s1, s2, s3, t0, t1, t2, t3, lhs, parents, octants, lead, out, w, x, edge, octs, sums):
    mine = pl.ds(table[32], 1)
    parent = parents[mine, :]
    live = (parent >= 0) & (parent < 768)
    target = jnp.where(live, parent - jnp.maximum(parent[:, :1], 0), -1)
    target = jnp.concatenate([target, lead[0:1]], axis=1)
    slot = lax.broadcasted_iota(jnp.int32, (ROWS, 512), 0)
    sums[...] = jnp.where(slot == target, 1.0, 0.0)[:, :LROWS].astype(BF)
    octant = jnp.concatenate([octants[mine, :], lead[1:2]], axis=1)
    which = lax.broadcasted_iota(jnp.int32, (128, 512), 0)
    hot = jnp.where(((which & 7) == octant) & (which < 16), 1.0, 0.0)
    octs[...] = hot.T[:LROWS, :16].astype(BF)
    for base, group in ((0, (s0, s1, s2, s3)), (16, (t0, t1, t2, t3))):
        n = 0
        for ref in group:
            for k in range(ref.shape[0]):
                w[table[base + n]] = ref[k]
                n += 1

    def product(p, _):
        wr = jnp.concatenate([w[2 * p, :KP, :], w[2 * p + 1, :KP, :]], axis=1)
        wi = jnp.concatenate([w[16 + 2 * p, :KP, :], w[17 + 2 * p, :KP, :]], axis=1)
        acc = jnp.dot(lhs[...], jnp.concatenate([wr, wi], axis=0), preferred_element_type=F32)
        acc = acc.astype(BF)
        x[2 * p + 1] = acc[:, :128]
        x[2 * p + 2] = acc[:, 128:]
        return 0

    lax.fori_loop(0, 8, product, 0, unroll=2)
    x[0] = x[16]
    x[17] = x[1]

    rows = lax.broadcasted_iota(jnp.int32, (256, 256), 0)
    cols = lax.broadcasted_iota(jnp.int32, (256, 256), 1)
    edge_row = (rows == 128) | (rows == 129) | (rows == 255)
    sample = jnp.where(rows < 128, rows, jnp.where(rows < 130, rows, jnp.where(rows == 255, -1, rows - 128)))
    tap = sample + 1 - cols // 2
    high_row = (rows < 128) | edge_row
    lane = lax.broadcasted_iota(jnp.int32, (2 * LROWS, 128), 1)
    row8 = lax.broadcasted_iota(jnp.int32, (8, 128), 0)
    sel_r = lax.broadcasted_iota(jnp.int32, (16, 512), 0)
    sel_c = lax.broadcasted_iota(jnp.int32, (16, 512), 1)
    pick = ((sel_r == 2) & (sel_c == 255)) | ((sel_r == 3) & (sel_c == 511))
    for r, c in ((12, 0), (13, 1), (14, 256), (15, 257)):
        pick = pick | ((sel_r == r) & (sel_c == c))
    pick = jnp.where(pick, 1.0, 0.0).astype(BF)

    def window(q, _):
        def row_of(base, t):
            both = w[base + q, 672:688, :].astype(F32)
            return jnp.concatenate([both[t : t + 1], both[4 + t : 5 + t]], axis=1)

        band = jnp.zeros((256, 256), F32)
        for t in range(4):
            band = jnp.where(tap == t, jnp.where(high_row, row_of(0, t), row_of(16, t)), band)

        def phases(base):
            both = jnp.concatenate([w[base + q, 640:656, :], w[base + q, 656:672, :]], axis=1)
            return jnp.dot(octs[...], both, preferred_element_type=F32)

        own = x[q + 1]
        side = jnp.where(lane < 2, x[q + 2], jnp.where(lane == 127, x[q], own))
        y = jnp.dot(jnp.concatenate([own, side], axis=1), band.astype(BF), preferred_element_type=F32)
        cos = phases(0)
        sin = phases(16)
        yr = y[:LROWS]
        yi = y[LROWS:]
        z = jnp.concatenate([yr * cos - yi * sin, yr * sin + yi * cos], axis=1)
        part = jnp.dot(sums[...], z.astype(BF), preferred_element_type=F32).astype(BF)
        out[q] = part
        ends = lax.dot_general(pick, part, (((1,), (1,)), ((), ())), preferred_element_type=F32)
        ends = jnp.concatenate([ends, jnp.zeros((16, 24), F32)], axis=1)
        edge[0, lax.rem(q + 1, 16)] = ends[:8]
        edge[1, lax.rem(q + 15, 16)] = ends[8:]
        return 0

    lax.fori_loop(0, 16, window, 0, unroll=4)

    def finish(q, _):
        last = out[q, 96:104, 0:128].astype(F32)
        out[q, 96:104, 0:128] = jnp.where(row8 < 2, last, edge[0, q] + edge[1, q]).astype(BF)
        return 0

    lax.fori_loop(0, 16, finish, 0)


def received(rows, recv, target):
    slot = lax.broadcasted_iota(jnp.int32, (rows, 16 * ROWS), 0)
    onehot = jnp.where(slot == target[...], 1.0, 0.0).astype(BF)
    sig = jnp.dot(onehot, recv[...], preferred_element_type=F32)
    ends = [recv[ROWS * a + 96 : ROWS * a + 104, 0:ROWS].astype(F32) for a in range(16)]
    ends = jnp.concatenate(ends, axis=1)
    ends = jnp.where(lax.broadcasted_iota(jnp.int32, (8, 16 * ROWS), 0) < 2, 0.0, ends).astype(BF)
    edge = lax.dot_general(ends, onehot, (((1,), (1,)), ((), ())), preferred_element_type=F32)
    return sig, jnp.concatenate([edge, edge], axis=0).astype(BF)


def raised(sig, halo, u_high, u_low, extras, octs, cos_t, sin_t):
    x = sig.astype(BF)

    def upsampled(part):
        src = x[:, 256 * part : 256 * part + 256]
        y = jnp.dot(src, u_high[...], preferred_element_type=F32)
        y = y + jnp.dot(src, u_low[...], preferred_element_type=F32)
        return y + lax.dot_general(halo, extras[part][...], (((0,), (0,)), ((), ())), preferred_element_type=F32)

    yr = upsampled(0)
    yi = upsampled(1)
    cos = jnp.dot(octs, cos_t[...], preferred_element_type=F32)
    sin = jnp.dot(octs, sin_t[...], preferred_element_type=F32)
    return yr * cos - yi * sin, yr * sin + yi * cos


def lead_kernel(recv, target, u_high, u_low, uh_re, uh_im, octs, cos_t, sin_t, mask, carry):
    sig, halo = received(16, recv, target)
    parts = raised(sig, halo, u_high, u_low, (uh_re, uh_im), octs[0:16], cos_t, sin_t)
    for part in range(2):
        total = jnp.sum(jnp.where(mask[...] > 0.5, parts[part], 0.0), axis=0, keepdims=True)
        for tile in range(4):
            carry[2 * tile + part : 2 * tile + part + 1, :] = total[:, 128 * tile : 128 * tile + 128]


def upper_kernel(recv, target, u_high, u_low, uh_re, uh_im, octs, cos_t, sin_t, sums, out1, out2):
    sig, halo = received(768, recv, target)
    for part in range(2):
        for tile in range(2):
            lanes = slice(256 * part + 128 * tile, 256 * part + 128 * tile + 128)
            out1[pl.ds(2 * tile + part, 768, stride=4), :] = sig[:, lanes]
    parts = raised(sig, halo, u_high, u_low, (uh_re, uh_im), octs[...], cos_t, sin_t)
    for part in range(2):
        z = parts[part]
        high = z.astype(BF)
        low = (z - high.astype(F32)).astype(BF)
        total = jnp.dot(sums[...], high, preferred_element_type=F32)
        total = total + jnp.dot(sums[...], low, preferred_element_type=F32)
        for tile in range(4):
            out2[pl.ds(2 * tile + part, 96, stride=8), :] = total[:, 128 * tile : 128 * tile + 128]


def vmem():
    return pl.BlockSpec(memory_space=pltpu.VMEM)


def body(
    coefficients,
    plane_map,
    leaf_parent,
    leaf_octant,
    box_parent,
    box_octant,
    interp_one,
    phase_one,
    interp_two,
    phase_two,
):
    place = lax.axis_index("angle")
    box = lax.axis_index("box")
    core = box % 2

    piece = pl.pallas_call(
        piece_kernel,
        out_shape=jax.ShapeDtypeStruct((PIECE, 128), BF),
        in_specs=[pl.BlockSpec(memory_space=pltpu.SMEM)] + [vmem()] * 3,
        out_specs=vmem(),
        compiler_params=pltpu.CompilerParams(vmem_limit_bytes=8 << 20),
        name="piece",
    )(core.reshape(1), plane_map, interp_one, phase_one)
    mine = gather_pieces(piece)
    theirs = [partner(m) for m in mine]

    steps = jnp.arange(16, dtype=jnp.int32)
    ahead = steps % 4
    across = steps // 4
    px, py = place // 4, place % 4

    def table_of(c):
        as_x = 4 * ((px + ahead) % 4) + (py + across) % 4
        as_y = 4 * ((px + across) % 4) + (py + ahead) % 4
        return 16 * c + jnp.where(c == 0, as_x, as_y)

    table = jnp.concatenate([table_of(core), table_of(1 - core), place.reshape(1)]).astype(jnp.int32)

    lead_flag = jnp.where(leaf_parent[:8] < 0, 1.0, 0.0).astype(BF)
    lead_oct = leaf_octant[:8].astype(BF)
    note = jnp.concatenate([lead_flag[:, None], lead_oct[:, None], jnp.zeros((8, KP - NCO - 2), BF)], axis=1)
    lead = jnp.transpose(coefficients[:, :, :8], (0, 2, 1))
    lead = jnp.concatenate([lead, jnp.stack([note, jnp.zeros_like(note)])], axis=2)
    lead = lax.ppermute(lead, ("box", "angle"), [(16 * (b + 1), 16 * b) for b in range(15)])
    coefficients, lead, leaf_parent, leaf_octant, box_parent, mine[0] = lax.optimization_barrier(
        (coefficients, lead, leaf_parent, leaf_octant, box_parent, mine[0])
    )
    slots_one = box_parent.shape[0]
    slots_two = slots_one // 8
    starts = jnp.maximum(leaf_parent[::CHUNK], 0)
    last_two = jnp.max(jnp.where(box_parent < slots_two, box_parent, -1))
    live_count = jnp.sum((box_parent != slots_two).astype(jnp.int32))
    rows = jnp.transpose(coefficients, (0, 2, 1))
    lead_flag = lead[0, :, NCO]
    lead_oct = lead[0, :, NCO + 1].astype(jnp.int32)
    lead = jnp.pad(lead[:, :, :NCO], ((0, 0), (0, LROWS - CHUNK - 8), (0, KP - NCO)))
    rows = jnp.concatenate([jnp.pad(rows, ((0, 0), (0, 0), (0, KP - NCO))), lead], axis=1)
    lhs = jnp.concatenate(
        [jnp.concatenate([rows[0], rows[1]], axis=0), jnp.concatenate([-rows[1], rows[0]], axis=0)], axis=1
    )

    lead_rows = jnp.stack([jnp.where(lead_flag > 0.5, CARRY, -1), lead_oct])
    lead_rows = jnp.pad(lead_rows, ((0, 0), (0, 120)), constant_values=-1)

    payload = pl.pallas_call(
        leaf_kernel,
        out_shape=jax.ShapeDtypeStruct((16, ROWS, 512), BF),
        in_specs=[pl.BlockSpec(memory_space=pltpu.SMEM)] + [vmem()] * 12,
        out_specs=vmem(),
        scratch_shapes=[pltpu.VMEM((32, PIECE, 128), BF), pltpu.VMEM((18, 2 * LROWS, 128), BF), pltpu.VMEM((2, 16, 8, 128), F32), pltpu.VMEM((LROWS, 16), BF), pltpu.VMEM((ROWS, LROWS), BF)],
        compiler_params=pltpu.CompilerParams(vmem_limit_bytes=28 << 20),
        name="leaf",
    )(table, *mine, *theirs, lhs, leaf_parent.reshape(16, CHUNK), leaf_octant.reshape(16, CHUNK), lead_rows)

    box_parent, box_octant, interp_two, phase_two, payload = lax.optimization_barrier(
        (box_parent, box_octant, interp_two, phase_two, payload)
    )
    recv = lax.all_to_all(payload, "angle", split_axis=0, concat_axis=0, tiled=True)

    row = jnp.arange(ROWS, dtype=jnp.int32)[None, :]
    slot = jnp.where(row < CARRY, starts[:, None] + row, -1)
    first_row = jnp.arange(16, dtype=jnp.int32)[:, None] == 0
    slot = jnp.where((row == CARRY) & first_row, live_count - 1, slot)

    col = jnp.arange(512, dtype=jnp.int32)[None, :] // 2

    def banded(sample):
        tap = sample[:, None] - col + 1
        full = jnp.zeros((sample.shape[0], 512), F32)
        for t in range(4):
            full = jnp.where(tap == t, interp_two[t][None, :], full)
        return split(full)

    u_high, u_low = banded(jnp.arange(256, dtype=jnp.int32))
    off = -1000
    re_high, re_low = banded(jnp.array([off, off, -1, off, 256, 257, off, off], jnp.int32))
    im_high, im_low = banded(jnp.array([off, off, off, -1, off, off, 256, 257], jnp.int32))
    cos_t = jnp.concatenate(split(jnp.cos(phase_two)), axis=0)
    sin_t = jnp.concatenate(split(jnp.sin(phase_two)), axis=0)
    octs_two = (box_octant[:, None] == jnp.arange(16, dtype=jnp.int32)[None, :] % 8).astype(BF)
    sums_two = (jnp.arange(slots_two, dtype=jnp.int32)[:, None] == box_parent[None, :]).astype(BF)
    lead_mask = jnp.broadcast_to((box_parent[:16, None] < 0).astype(F32), (16, 512))

    operands = (
        recv.reshape(16 * ROWS, 512),
        slot.reshape(1, 16 * ROWS),
        u_high,
        u_low,
        jnp.concatenate([re_high, re_low], axis=0),
        jnp.concatenate([im_high, im_low], axis=0),
        octs_two,
        cos_t,
        sin_t,
    )
    carry = pl.pallas_call(
        lead_kernel,
        out_shape=jax.ShapeDtypeStruct((8, 128), F32),
        in_specs=[vmem()] * 10,
        out_specs=vmem(),
        compiler_params=pltpu.CompilerParams(vmem_limit_bytes=16 << 20),
        name="lead",
    )(*operands, lead_mask)
    incoming = lax.ppermute(carry, "box", [(i + 1, i) for i in range(15)])
    out1, out2 = pl.pallas_call(
        upper_kernel,
        out_shape=(jax.ShapeDtypeStruct((3072, 128), F32), jax.ShapeDtypeStruct((768, 128), F32)),
        in_specs=[vmem()] * 10,
        out_specs=(vmem(), vmem()),
        compiler_params=pltpu.CompilerParams(vmem_limit_bytes=28 << 20),
        name="upper",
    )(*operands, sums_two)
    signature_one = out1.reshape(768, 2, 2, 128).transpose(0, 2, 1, 3).reshape(768, 2, 256)
    incoming = jnp.where(last_two < 0, 0.0, incoming)
    at = 8 * jnp.maximum(last_two, 0)
    out2 = lax.dynamic_update_slice_in_dim(out2, lax.dynamic_slice_in_dim(out2, at, 8, 0) + incoming, at, 0)
    signature_two = out2.reshape(96, 4, 2, 128).transpose(0, 2, 1, 3).reshape(96, 2, 512)
    return (signature_one, signature_two)


def solution(mesh):
    in_specs = (
        P(None, None, ("box", "angle")),
        P(None, None, "angle"),
        P("box"),
        P("box"),
        P("box"),
        P("box"),
        P(None, "angle"),
        P(None, "angle"),
        P(None, "angle"),
        P(None, "angle"),
    )
    out_specs = (P("box", None, "angle"), P("box", None, "angle"))
    return jax.shard_map(body, mesh=mesh, in_specs=in_specs, out_specs=out_specs, check_vma=False)
```
